256 devices in a mesh: section: 8 (over z_lo, x), dp: 32 (over z_hi, y, core).
Axes of the slice: x: 4, y: 4, z: 8 (z_hi: 4, z_lo: 2; z = z_hi * 2 + z_lo), core: 2. Of those that a mesh axis runs over, the one named last changes fastest.
Arguments:
- activations: bfloat16 [8, 8, 1536, 5376], P('section', None, 'dp'), may hold values from -6 to 6
- loss_grads: bfloat16 [8, 1536, 5376], P(None, 'dp'), may hold values from -6 to 6
- adapter_in: bfloat16 [8, 5376, 64], P('section'), may hold values from -0.078125 to 0.078125
- adapter_out: bfloat16 [8, 64, 5376], P('section'), may hold values from -0.75 to 0.75
- first_moment: float32 [8, 32, 43008], P('section', 'dp'), may hold values from -0.4 to 0.4
- second_moment: float32 [8, 32, 43008], P('section', 'dp'), may hold values from 0.0001 to 0.01
- old_owner: int32 [8, 16], P('section'), may hold values from 0 to 31, as said below
- new_owner: int32 [8, 32], P('section'), may hold values from 0 to 31, each once within a row
- plan: int32 [8], replicated, may hold values from 0 to 7, each once
Outputs:
- input_grads: bfloat16 [8, 8, 1536, 5376], P('section', None, 'dp')
- adam_update: float32 [8, 32, 21504], P('section', 'dp')
- first_new: float32 [8, 32, 21504], P('section', 'dp')
- second_new: float32 [8, 32, 21504], P('section', 'dp')
The draws below stay inside these ranges and needn't reach their ends.
Inputs may be any that keep to these rules, and one draw needn't show every extreme that they name: `old_owner`: the entries of one section's row are distinct.
All inputs are finite; a program needn't handle non-finite values.
Results may differ from the reference program's by a relative error of at most 0.025.
Values may be sent and summed in bfloat16 or wider, within the bound.
A program may use at most 64 MiB of HBM per device.

```python
import math
import jax
import jax.numpy as jnp

D = 5376
RANK = 64
MB = 8
SECTIONS = 8
TOKENS = 1536
BLOCK = 21504
OLD_DP = 16
N_DP = 32


def draw_old_owner(key, part):
    section_keys = jax.random.split(key, SECTIONS)
    rows = jax.vmap(lambda section_key: jax.random.permutation(section_key, N_DP)[:OLD_DP])(section_keys)
    return rows.astype(jnp.int32)


def strengthened(drawn, key, source, target, parts, factor):
    owner, partner = [(jnp.arange(drawn.shape[axis_at]) // (drawn.shape[axis_at] // parts)).reshape([-1 if axis == axis_at else 1 for axis in range(drawn.ndim)]) for axis_at in (source, target)]
    chosen = jax.random.permutation(key, parts)[partner]
    strong = (owner == chosen) | (owner == (partner + parts // 2) % parts)
    return jnp.where(strong, factor * drawn, drawn)


def levels(key, shape, cuts, low, largest):
    loudness, own = 1.0, jax.random.fold_in(key, 6)
    for dim, blocks in cuts:
        steps = jnp.exp(jax.random.uniform(jax.random.fold_in(own, dim), (blocks,), jnp.float32, low / len(cuts), largest / len(cuts)))
        loudness = loudness * jnp.repeat(steps, shape[dim] // blocks).reshape([-1 if axis == dim else 1 for axis in range(len(shape))])
    return loudness


def bell_draw(stream_key, shape, width, bound, cuts=(), kind=jnp.bfloat16):
    array = jax.random.normal(stream_key, shape, jnp.float32) * width
    if len(cuts) > 0:
        array = levels(stream_key, shape, cuts, -0.22, 0.18) * array
    return jnp.clip(array, min=-bound, max=bound).astype(kind)


def heavy_noise(rng, dims, width, reach, shards, heavy, kind=jnp.bfloat16):
    array = width * jax.random.normal(rng, dims, jnp.float32)
    if shards:
        array = array * levels(rng, dims, shards, -0.22, 0.18)
    return jnp.clip(strengthened(array, jax.random.fold_in(rng, 3), *heavy), -reach, reach).astype(kind)


def setup_inputs(seed: int = 0) -> dict:
    key_of = jax.random.split(jax.random.key(seed), 10)
    activations = bell_draw(key_of[0], (SECTIONS, MB, TOKENS, D), 1.0, 6.0, ((0, 8), (2, 32)))
    loss_grads = heavy_noise(key_of[1], (MB, TOKENS, D), 1.0, 6.0, ((1, 32),), (1, 2, 32, 2.75))
    adapter_in = bell_draw(key_of[2], (SECTIONS, D, RANK), D ** -0.5, 0.078125, ((0, 8),))
    adapter_out = bell_draw(key_of[3], (SECTIONS, RANK, D), RANK ** -0.5, 0.75, ((0, 8),))
    first_moment = bell_draw(key_of[4], (SECTIONS, N_DP, 2 * BLOCK), 0.05, 0.4, ((0, 8), (1, 32)), jnp.float32)
    second_moment = jnp.clip(jnp.exp(math.log(0.01) - 4.6051702 * jax.random.uniform(key_of[5], (SECTIONS, N_DP, 2 * BLOCK), jnp.float32) ** levels(key_of[5], (SECTIONS, N_DP, 2 * BLOCK), ((0, 8), (1, 32)), -0.2, 0.2)), 0.0001, 0.01)
    old_owner = draw_old_owner(jax.random.fold_in(key_of[9], 71), 0)
    new_owner = jax.vmap(lambda own: jax.random.permutation(own, N_DP))(jax.random.split(key_of[7], SECTIONS)).reshape((SECTIONS, N_DP)).astype(jnp.int32)
    plan = jax.random.permutation(key_of[8], MB).astype(jnp.int32)
    return dict(activations=activations, loss_grads=loss_grads, adapter_in=adapter_in, adapter_out=adapter_out, first_moment=first_moment, second_moment=second_moment, old_owner=old_owner, new_owner=new_owner, plan=plan)


beta_one = 0.9
beta_two = 0.95
adam_eps = 1e-08
adam_step = 1000.0
loss_scale = 4096.0

def silu_slope(pre_value):
    gate_value = jax.nn.sigmoid(pre_value)
    return gate_value * (1.0 + pre_value * (1.0 - gate_value))

def adam_rows(grads, first, second):
    first_next = beta_one * first + (1.0 - beta_one) * grads
    second_next = beta_two * second + (1.0 - beta_two) * grads * grads
    update = first_next / (1.0 - beta_one ** adam_step) / (jnp.sqrt(second_next / (1.0 - beta_two ** adam_step)) + adam_eps)
    return (update, first_next, second_next)

def reference(activations, loss_grads, adapter_in, adapter_out, first_moment, second_moment, old_owner, new_owner, plan):
    incoming = loss_grads[plan]
    emitted = []
    updates = []
    firsts = []
    seconds = []
    for section_index in reversed(range(SECTIONS)):
        section_input = activations[section_index][plan].reshape(-1, D)
        incoming_flat = incoming.reshape(-1, D)
        weight_in = adapter_in[section_index]
        weight_out = adapter_out[section_index]
        pre_value = jnp.dot(section_input, weight_in, preferred_element_type=jnp.float32)
        hidden = jax.nn.silu(pre_value).astype(jnp.bfloat16)
        act_grad = jnp.dot(incoming_flat, weight_out.T, preferred_element_type=jnp.float32)
        pre_grad = (act_grad * silu_slope(pre_value)).astype(jnp.bfloat16)
        input_grad = (incoming_flat.astype(jnp.float32) + jnp.dot(pre_grad, weight_in.T, preferred_element_type=jnp.float32)).astype(jnp.bfloat16)
        grad_in = jnp.dot(section_input.T, pre_grad, preferred_element_type=jnp.float32)
        grad_out = jnp.dot(hidden.T, incoming_flat, preferred_element_type=jnp.float32)
        grads = jnp.concatenate([grad_in.reshape(-1), grad_out.reshape(-1)]) / loss_scale
        first_old = first_moment[section_index][old_owner[section_index]].reshape(-1)
        second_old = second_moment[section_index][old_owner[section_index]].reshape(-1)
        update, first_next, second_next = adam_rows(grads, first_old, second_old)
        inverse = jnp.argsort(new_owner[section_index]).astype(jnp.int32)
        updates.insert(0, update.reshape(N_DP, BLOCK)[inverse])
        firsts.insert(0, first_next.reshape(N_DP, BLOCK)[inverse])
        seconds.insert(0, second_next.reshape(N_DP, BLOCK)[inverse])
        incoming = input_grad.reshape(MB, TOKENS, D)
        emitted.insert(0, incoming)
    return (jnp.stack(emitted), jnp.stack(updates), jnp.stack(firsts), jnp.stack(seconds))
```

```python
import functools

import jax
import jax.numpy as jnp
from jax import lax
from jax.experimental import pallas as pl
from jax.experimental.pallas import tpu as pltpu
from jax.sharding import Mesh
from jax.sharding import PartitionSpec as P

DP = ("dp_0", "dp_1", "dp_2")
ND, NY, NC = 4, 4, 2
SECTIONS = 8
RELAYS = 7
ALONG_Z = (1, 3, 5)
MESH = pl.DeviceIdType.MESH
BF = jnp.bfloat16
F32 = jnp.float32

beta_one = 0.9
beta_two = 0.95
adam_eps = 1e-08
adam_step = 1000.0
loss_scale = 4096.0


def dp_coords(index):
    return {"dp_0": index // (NY * NC), "dp_1": lax.rem(index // NC, NY), "dp_2": lax.rem(index, NC)}


def relay_spot(index):
    return 4 * index + index % 4


def drain_kernel(
    table_ref,
    inputs_ref,
    base_ref,
    turned_ref,
    rows_ref,
    weight_in_ref,
    weight_out_ref,
    first_ref,
    second_ref,
    p_ref,
    moved_ref,
    whole_ref,
    sum_ref,
    inputs,
    base,
    pre_sum,
    act_sum,
    hidden,
    rows_got,
    packed,
    prod,
    uv_out,
    uv_got,
    total,
    spread,
    picked,
    grad,
    flat,
    mixed_rows,
    held,
    half_out,
    half_got,
    y_out,
    y_got,
    z_out,
    z_got,
    load_sem,
    rows_send,
    rows_recv,
    prod_send,
    prod_recv,
    uv_send,
    uv_recv,
    gather_send,
    gather_recv,
    p_send,
    p_recv,
    spread_send,
    spread_recv,
    moved_send,
    moved_recv,
    slice_send,
    slice_recv,
    wide_send,
    wide_recv,
    pair_send,
    pair_recv,
    half_send,
    half_recv,
    y_send,
    y_recv,
    z_send,
    z_recv,
):
    sections = SECTIONS
    replicas = ND * NY * NC
    me = lax.axis_index("section")
    z = lax.axis_index("dp_0")
    y = lax.axis_index("dp_1")
    core = lax.axis_index("dp_2")
    dp = (z * NY + y) * NC + core
    other = 1 - core
    tokens, width = inputs.shape
    rank = weight_in_ref.shape[0]
    tok_rows = tokens // sections
    lanes = sections * rank
    parts = load_sem.shape[1]
    chunk = width // parts
    groups = chunk // 128
    block_rows = flat.shape[0] // (replicas // 2)
    half_blocks = replicas // 2
    extra = held.shape[1] - block_rows

    def load(which, part):
        source, target = ((inputs_ref, inputs), (base_ref, base))[which]
        columns = pl.ds(pl.multiple_of(part * chunk, 128), chunk)
        return pltpu.make_async_copy(
            source.at[:, columns], target.at[:, columns], load_sem.at[which, part]
        )

    for part in range(parts):
        load(0, part).start()
        load(1, part).start()

    barrier = pltpu.get_barrier_semaphore()
    for step in range(1, sections):
        pl.semaphore_signal(
            barrier, inc=1, device_id={"section": lax.rem(me + step, sections)}, device_id_type=MESH
        )

    def greet(step, carry):
        pl.semaphore_signal(
            barrier, inc=1, device_id=dp_coords(lax.rem(dp + step, replicas)), device_id_type=MESH
        )
        return carry

    lax.fori_loop(1, replicas, greet, 0)
    pl.semaphore_wait(barrier, sections - 1 + replicas - 1)

    def section_copy(src, dst, send, recv, target):
        return pltpu.make_async_remote_copy(
            src_ref=src,
            dst_ref=dst,
            send_sem=send,
            recv_sem=recv,
            device_id={"section": target},
            device_id_type=MESH,
        )

    def took(view, sem):
        section_copy(view, view, sem, sem, me).wait_recv()

    def sent(view, sem):
        section_copy(view, view, sem, sem, me).wait_send()

    hop = dp // 4

    def rows_copy():
        return section_copy(
            rows_ref.at[:, lax.rem(dp, 4)],
            rows_got,
            rows_send,
            rows_recv,
            lax.rem(me + sections - hop, sections),
        )

    @pl.when(me < hop)
    def _():
        rows_copy().start()

    def along_z(section):
        return lax.rem(section, 2) * (1 - section // 7)

    def row_of(section):
        return y + along_z(section) * (z - y)

    for section in range(1, sections):

        @pl.when(me == section)
        def _(section=section):
            row = z if section in ALONG_Z else y
            for target in reversed(range(section)):
                section_copy(
                    turned_ref.at[row, core],
                    whole_ref.at[section, row, core],
                    slice_send,
                    slice_recv.at[section],
                    target,
                ).start()

    relay = dp // 4
    is_relay = (lax.rem(dp, 4) == lax.rem(relay, 4)) & (relay < RELAYS)

    def spread_copy(which, index):
        source = first_ref if which == 0 else second_ref
        peer = relay_spot(index)
        return pltpu.make_async_remote_copy(
            src_ref=source.at[:, index],
            dst_ref=spread.at[dp, which],
            send_sem=spread_send,
            recv_sem=spread_recv,
            device_id={"dp_0": peer // 8, "dp_1": peer // 2 % 4, "dp_2": peer % 2},
            device_id_type=MESH,
        )

    for index in range(RELAYS):

        @pl.when(dp != relay_spot(index))
        def _(index=index):
            spread_copy(0, index).start()
            spread_copy(1, index).start()

        @pl.when(dp == relay_spot(index))
        def _(index=index):
            spread[relay_spot(index), 0] = first_ref[:, index]
            spread[relay_spot(index), 1] = second_ref[:, index]

    across = (((1,), (1,)), ((), ()))
    down = (((0,), (0,)), ((), ()))
    pre_sum[...] = jnp.zeros_like(pre_sum)
    act_sum[...] = jnp.zeros_like(act_sum)

    def accumulate(part, carry):
        columns = pl.ds(pl.multiple_of(part * chunk, 128), chunk)
        load(0, part).wait()
        pre_sum[...] += lax.dot_general(
            inputs[:, columns], weight_in_ref[:, columns], across, preferred_element_type=F32
        )
        load(1, part).wait()
        act_sum[...] += lax.dot_general(
            base[:, columns], weight_out_ref[:, columns], across, preferred_element_type=F32
        )
        return carry

    lax.fori_loop(0, parts, accumulate, 0)
    pre_value = pre_sum[...]
    gate = jax.nn.sigmoid(pre_value)
    hidden[...] = (pre_value * gate).astype(BF)
    slope = gate * (1.0 + pre_value * (1.0 - gate))
    both = jnp.concatenate([act_sum[...].astype(BF), slope.astype(BF)], axis=1)
    uv_out[...] = both.reshape(sections, tok_rows, 2 * rank)

    def uv_copy(step):
        target = lax.rem(me + step, sections)
        return section_copy(uv_out.at[target], uv_got.at[me], uv_send, uv_recv, target)

    for step in range(1, sections):
        uv_copy(step).start()
    uv_got[me] = uv_out[me]

    slot = lax.rem(hop + me, sections) * 4 + lax.rem(dp, 4)
    valid = me + hop >= sections

    def prod_copy(step):
        return pltpu.make_async_remote_copy(
            src_ref=packed,
            dst_ref=prod.at[me, slot],
            send_sem=prod_send,
            recv_sem=prod_recv,
            device_id=dp_coords(lax.rem(dp + step, replicas)),
            device_id_type=MESH,
        )

    @pl.when(valid)
    def _():
        took(rows_got, rows_recv)
        pieces = [
            lax.dot_general(rows_got[k], weight_in_ref[...], across, preferred_element_type=F32)
            for k in range(2)
        ]
        packed[...] = jnp.concatenate(pieces, axis=1).astype(BF)

        def prod_start(step, carry):
            prod_copy(step).start()
            return carry

        lax.fori_loop(1, replicas, prod_start, 0)
        prod[me, slot] = packed[...]

    def outward(part, carry):
        columns = pl.ds(pl.multiple_of(part * chunk, 128), chunk)
        result = lax.dot_general(hidden[...], base[:, columns], down, preferred_element_type=F32)
        for group in range(groups):
            flat[pl.ds(part * groups + group, rank, stride=width // 128), :] = result[
                :, group * 128 : (group + 1) * 128
            ]
        return carry

    lax.fori_loop(0, parts, outward, 0)
    for block in range(half_blocks):
        held[half_blocks + block, :block_rows] = flat[pl.ds(block * block_rows, block_rows), :]

    for section in range(1, sections):

        @pl.when((me == section) & valid)
        def _(section=section):
            took(prod.at[0, pl.ds(0, 4 * section - 1)], prod_recv)

        @pl.when((me == section) & (me + hop < sections))
        def _(section=section):
            took(prod.at[0, pl.ds(0, 4 * section)], prod_recv)

        @pl.when(me == section)
        def _(section=section):
            for step in range(1, sections):
                section_copy(
                    prod.at[section, pl.ds(0, 4 * section)],
                    prod.at[section, pl.ds(0, 4 * section)],
                    gather_send,
                    gather_recv.at[section],
                    (section - step) % sections,
                ).start()

    def wide_copy(section, shift):
        view = whole_ref.at[section, row_of(section), core]
        axis, at, count = ("dp_0", z, ND) if section in ALONG_Z else ("dp_1", y, NY)
        return pltpu.make_async_remote_copy(
            src_ref=view,
            dst_ref=view,
            send_sem=wide_send.at[section],
            recv_sem=wide_recv.at[section],
            device_id={axis: lax.rem(at + shift, count)},
            device_id_type=MESH,
        )

    for section in range(1, sections):

        @pl.when(me < section)
        def _(section=section):
            took(whole_ref.at[section, row_of(section), core], slice_recv.at[section])
            for shift in (1, 3, 2):
                wide_copy(section, shift).start()

    def moved_copy(step):
        peer = lax.rem(dp + step, replicas)
        return pltpu.make_async_remote_copy(
            src_ref=picked.at[peer],
            dst_ref=moved_ref.at[:, relay],
            send_sem=moved_send,
            recv_sem=moved_recv,
            device_id=dp_coords(peer),
            device_id_type=MESH,
        )

    @pl.when(is_relay)
    def _():
        took(spread.at[pl.ds(0, replicas - 1)], spread_recv)

        def pick(target, carry):
            owner = table_ref[0, target]
            half = table_ref[1, target]
            picked[target, 0] = spread[owner, 0, half]
            picked[target, 1] = spread[owner, 1, half]
            return carry

        lax.fori_loop(0, replicas, pick, 0)

        def moved_start(step, carry):
            moved_copy(step).start()
            return carry

        lax.fori_loop(1, replicas, moved_start, 0)
        moved_ref[:, relay] = picked[dp]

    took(uv_got.at[pl.ds(0, sections - 1)], uv_recv)
    for section in range(1, sections):

        @pl.when(me != section)
        def _(section=section):
            took(prod.at[section, pl.ds(0, 4 * section)], gather_recv.at[section])

    total[...] = jnp.zeros_like(total)
    for turn in reversed(range(sections)):
        low, high = turn * rank, (turn + 1) * rank
        pair = uv_got[turn].astype(F32)
        p_value = ((pair[:, :rank] + total[:, low:high]) * pair[:, rank:]).astype(BF)
        p_ref[me, :, low:high] = p_value
        if turn:
            got = prod[turn, : 4 * turn].astype(F32).reshape(turn, 32, 2 * rank)
            rows = jnp.concatenate([got[:, :, :rank], got[:, :, rank:]], axis=1)
            rows = rows.reshape(turn * rank, rank).astype(BF)
            total[:, :low] += lax.dot_general(p_value, rows, across, preferred_element_type=F32)

    def live(section):
        start = section // 2 * 2 * rank
        return pl.ds(start, lanes - start)

    def p_copy(section):
        view = p_ref.at[me, :, live(section)]
        return section_copy(view, view, p_send.at[section], p_recv, section)

    for section in range(sections):

        @pl.when(me != section)
        def _(section=section):
            p_copy(section).start()

    for section in range(sections):

        @pl.when(me == section)
        def _(section=section):
            took(p_ref.at[pl.ds(0, sections - 1), :, live(section)], p_recv)

    lane_section = lax.broadcasted_iota(jnp.int32, (tokens, lanes), 1) // rank
    p_all = p_ref[...].reshape(tokens, lanes)
    p_above = jnp.where(lane_section > me, p_all, jnp.zeros_like(p_all))
    p_live = jnp.where(lane_section == me, p_all, jnp.zeros_like(p_all))
    take = lax.rem(lax.broadcasted_iota(jnp.int32, (lanes, rank), 0), rank) == (
        lax.broadcasted_iota(jnp.int32, (lanes, rank), 1)
    )
    p_mine = jnp.dot(p_live, take.astype(F32).astype(BF), preferred_element_type=F32).astype(BF)

    def inward(part, carry):
        columns = pl.ds(pl.multiple_of(part * chunk, 128), chunk)
        grad[columns, :] = lax.dot_general(
            inputs[:, columns], p_mine, down, preferred_element_type=F32
        )
        return carry

    lax.fori_loop(0, parts, inward, 0)
    mixed = lax.dot_general(hidden[...], p_above, down, preferred_element_type=F32)
    for group in range(lanes // 128):
        mixed_rows[pl.ds(group, rank, stride=lanes // 128), :] = mixed[
            :, group * 128 : (group + 1) * 128
        ]
    for block in range(half_blocks):
        even = grad[pl.ds(block * 2 * block_rows, block_rows, stride=2), :]
        odd = grad[pl.ds(block * 2 * block_rows + 1, block_rows, stride=2), :]
        held[block, :block_rows] = jnp.concatenate([even, odd], axis=1)
        held[block, block_rows:] = jnp.zeros((extra, 128), F32)
        held[half_blocks + block, block_rows:] = mixed_rows[pl.ds(block * extra, extra), :]

    order = (2, 1, 3, 0)

    def half_copy(far):
        return pltpu.make_async_remote_copy(
            src_ref=half_out.at[far],
            dst_ref=half_got.at[far],
            send_sem=half_send.at[far],
            recv_sem=half_recv.at[far],
            device_id={"dp_2": other},
            device_id_type=MESH,
        )

    def y_copy(far, step):
        there = lax.rem(y + step, NY)
        return pltpu.make_async_remote_copy(
            src_ref=y_out.at[far, there],
            dst_ref=y_got.at[far, step],
            send_sem=y_send.at[far],
            recv_sem=y_recv.at[far],
            device_id={"dp_1": there},
            device_id_type=MESH,
        )

    def z_copy(far):
        return pltpu.make_async_remote_copy(
            src_ref=z_out.at[far],
            dst_ref=z_got.at[far],
            send_sem=z_send.at[far],
            recv_sem=z_recv.at[far],
            device_id={"dp_0": lax.rem(z + far, ND)},
            device_id_type=MESH,
        )

    for far in order:
        there = lax.rem(z + far, ND)
        for column in range(NY):
            half_out[far, column] = held[table_ref[2, (other * ND + there) * NY + column]].astype(BF)
        half_copy(far).start()
    for far in order:
        there = lax.rem(z + far, ND)
        half_copy(far).wait_recv()
        for column in range(NY):
            own = held[table_ref[2, (core * ND + there) * NY + column]]
            y_out[far, column] = (own + half_got[far, column].astype(F32)).astype(BF)
        for step in (2, 1, 3):
            y_copy(far, step).start()
    for far in order:
        took(y_got.at[far, pl.ds(1, NY - 1)], y_recv.at[far])
        part = y_out[far, y].astype(F32)
        for step in range(1, NY):
            part += y_got[far, step].astype(F32)
        if far:
            z_out[far] = part.astype(BF)
            z_copy(far).start()
        else:
            sum_ref[...] = part

    def pair_copy(section):
        view = whole_ref.at[section, :, core]
        return pltpu.make_async_remote_copy(
            src_ref=view,
            dst_ref=view,
            send_sem=pair_send.at[section],
            recv_sem=pair_recv.at[section],
            device_id={"dp_2": other},
            device_id_type=MESH,
        )

    for section in reversed(range(1, sections)):

        @pl.when(me < section)
        def _(section=section):
            took(whole_ref.at[section, pl.ds(0, 3), core], wide_recv.at[section])
            pair_copy(section).start()

    for far in range(1, ND):
        z_copy(far).wait_recv()
    result = sum_ref[...]
    for far in range(1, ND):
        result += z_got[far].astype(F32)
    sum_ref[...] = result

    @pl.when(is_relay)
    def _():
        took(moved_ref.at[:, pl.ds(0, RELAYS - 1)], moved_recv)
        sent(picked.at[pl.ds(0, replicas - 1)], moved_send)
        sent(spread.at[pl.ds(0, RELAYS - 1)], spread_send)

    @pl.when(jnp.logical_not(is_relay))
    def _():
        took(moved_ref, moved_recv)
        sent(spread.at[pl.ds(0, RELAYS)], spread_send)

    @pl.when(me < hop)
    def _():
        rows_copy().wait_send()

    @pl.when(valid)
    def _():
        sent(prod.at[0, pl.ds(0, replicas - 1)], prod_send)

    sent(uv_out.at[pl.ds(0, sections - 1)], uv_send)
    for section in range(sections):

        @pl.when(me != section)
        def _(section=section):
            p_copy(section).wait_send()

    for section in range(1, sections):

        @pl.when(me == section)
        def _(section=section):
            sent(prod.at[pl.ds(0, sections - 1), pl.ds(0, 4 * section)], gather_send)
            sent(whole_ref.at[pl.ds(0, section), 0, 0], slice_send)

        @pl.when(me < section)
        def _(section=section):
            sent(whole_ref.at[section, pl.ds(0, 3), core], wide_send.at[section])
            pair_copy(section).wait()

    for far in range(ND):
        half_copy(far).wait_send()
        sent(y_got.at[far, pl.ds(1, NY - 1)], y_send.at[far])
        if far:
            z_copy(far).wait_send()


def final_kernel(
    spots_ref,
    base_ref,
    p_ref,
    whole_ref,
    own_ref,
    summed_ref,
    moved_ref,
    emitted_ref,
    update_ref,
    first_ref,
    second_ref,
    left,
    weights,
    extra,
):
    step = pl.program_id(0)
    section = spots_ref[0]
    my_block = spots_ref[1]
    micro_count, tok_rows, chunk = base_ref.shape
    lanes = p_ref.shape[2]
    tokens = micro_count * tok_rows
    rank = own_ref.shape[0]
    rows = update_ref.shape[0]
    groups = lanes // 128

    @pl.when(step == 0)
    def _():
        lane_section = lax.broadcasted_iota(jnp.int32, (tok_rows, lanes), 1) // rank
        for micro in range(micro_count):
            value = p_ref[spots_ref[2 + micro]]
            left[micro * tok_rows : (micro + 1) * tok_rows, :] = jnp.where(
                lane_section >= section, value, jnp.zeros_like(value)
            )
        mixed = jnp.concatenate(
            [summed_ref[pl.ds(rows + group, 4, stride=groups), :] for group in range(groups)],
            axis=1,
        )
        mixed = jnp.concatenate([mixed, jnp.zeros((12, lanes), F32)], axis=0)
        left[tokens:, :] = mixed.astype(BF)

    for place in range(lanes // rank):
        part = pl.ds(place * rank, rank)

        @pl.when(place < section)
        def _(part=part):
            weights[part, :] = jnp.zeros((rank, chunk), BF)

        @pl.when(place == section)
        def _(part=part):
            weights[part, :] = own_ref[...]

        @pl.when(place > section)
        def _(part=part):
            weights[part, :] = whole_ref[part, :]

    result = jnp.dot(left[...], weights[...], preferred_element_type=F32)
    for micro in range(micro_count):
        moved = result[micro * tok_rows : (micro + 1) * tok_rows]
        emitted_ref[micro] = (base_ref[spots_ref[2 + micro]].astype(F32) + moved).astype(BF)
    added = result[tokens : tokens + 4]
    for group in range(chunk // 128):
        extra[pl.ds(step * (chunk // 128) + group, 4, stride=rows // 4), :] = added[
            :, group * 128 : (group + 1) * 128
        ]

    @pl.when(step == pl.num_programs(0) - 1)
    def _():
        outward = (my_block >= NC * NY * ND // 2).astype(F32)
        main = summed_ref[:rows, :]
        grads = jnp.where(outward > 0, main + extra[...], main) / loss_scale
        first_next = beta_one * moved_ref[0] + (1.0 - beta_one) * grads
        second_next = beta_two * moved_ref[1] + (1.0 - beta_two) * grads * grads
        first_ref[...] = first_next
        second_ref[...] = second_next
        update_ref[...] = (
            first_next
            / (1.0 - beta_one**adam_step)
            / (jnp.sqrt(second_next / (1.0 - beta_two**adam_step)) + adam_eps)
        )


def vmem():
    return pl.BlockSpec(memory_space=pltpu.VMEM)


def smem():
    return pl.BlockSpec(memory_space=pltpu.SMEM)


def hbm():
    return pl.BlockSpec(memory_space=pl.ANY)


def run_drain(table, inputs, base, turned, weight_out, first, second):
    tokens, width = inputs.shape
    rank = turned.shape[0]
    sections = SECTIONS
    replicas = ND * NY * NC
    tok_rows = tokens // sections
    lanes = sections * rank
    half_blocks = replicas // 2
    rows = width * rank // half_blocks // 128
    extra = rank * lanes // 128 // half_blocks
    relay_rows = first.shape[2]
    dma = pltpu.SemaphoreType.DMA
    full = (rows + extra, 128)
    return pl.pallas_call(
        drain_kernel,
        out_shape=(
            jax.ShapeDtypeStruct((sections, tok_rows, lanes), BF),
            jax.ShapeDtypeStruct((2, RELAYS, relay_rows, 128), F32),
            jax.ShapeDtypeStruct((sections, NY, NC, 8, width), BF),
            jax.ShapeDtypeStruct(full, F32),
        ),
        in_specs=[smem()] + [hbm()] * 4 + [vmem()] * 4,
        out_specs=(vmem(), vmem(), hbm(), vmem()),
        scratch_shapes=[
            pltpu.VMEM((tokens, width), BF),
            pltpu.VMEM((tokens, width), BF),
            pltpu.VMEM((tokens, rank), F32),
            pltpu.VMEM((tokens, rank), F32),
            pltpu.VMEM((tokens, rank), BF),
            pltpu.VMEM((2, 8, width), BF),
            pltpu.VMEM((8, 128), BF),
            pltpu.VMEM((sections, 32, 8, 128), BF),
            pltpu.VMEM((sections, tok_rows, 2 * rank), BF),
            pltpu.VMEM((sections, tok_rows, 2 * rank), BF),
            pltpu.VMEM((tok_rows, lanes), F32),
            pltpu.VMEM((replicas, 2, 2, relay_rows, 128), F32),
            pltpu.VMEM((replicas, 2, relay_rows, 128), F32),
            pltpu.VMEM((width, rank), F32),
            pltpu.VMEM((half_blocks * rows, 128), F32),
            pltpu.VMEM((half_blocks * extra, 128), F32),
            pltpu.VMEM((replicas, *full), F32),
            pltpu.VMEM((ND, NY, *full), BF),
            pltpu.VMEM((ND, NY, *full), BF),
            pltpu.VMEM((ND, NY, *full), BF),
            pltpu.VMEM((ND, NY, *full), BF),
            pltpu.VMEM((ND, *full), BF),
            pltpu.VMEM((ND, *full), BF),
            dma((2, 6)),
            dma,
            dma,
            dma,
            dma,
            dma,
            dma,
            dma,
            dma((sections,)),
            dma((sections,)),
            dma,
            dma,
            dma,
            dma,
            dma,
            dma,
            dma((sections,)),
            dma((sections,)),
            dma((sections,)),
            dma((sections,)),
            dma((sections,)),
            dma((ND,)),
            dma((ND,)),
            dma((ND,)),
            dma((ND,)),
            dma((ND,)),
            dma((ND,)),
        ],
        compiler_params=pltpu.CompilerParams(
            collective_id=0, has_side_effects=True, vmem_limit_bytes=60 * 2**20
        ),
        name="drain",
    )(
        table,
        inputs,
        base,
        turned.reshape(NY, NC, 8, width),
        weight_out.reshape(2, rank // 16, 8, width),
        turned,
        weight_out,
        first,
        second,
    )


def run_final(spots, base, p_all, whole, own, summed, moved):
    micro_count, tok_rows, width = base.shape
    lanes = p_all.shape[2]
    tokens = micro_count * tok_rows
    rank = own.shape[0]
    rows = moved.shape[1]
    steps = 7
    chunk = width // steps
    row_shape = jax.ShapeDtypeStruct((rows, 128), F32)
    row_spec = pl.BlockSpec((rows, 128), lambda i: (0, 0))
    return pl.pallas_call(
        final_kernel,
        grid=(steps,),
        out_shape=(
            jax.ShapeDtypeStruct((micro_count, tok_rows, width), BF),
            row_shape,
            row_shape,
            row_shape,
        ),
        in_specs=[
            smem(),
            pl.BlockSpec((micro_count, tok_rows, chunk), lambda i: (0, 0, i)),
            pl.BlockSpec(p_all.shape, lambda i: (0, 0, 0)),
            pl.BlockSpec((lanes, chunk), lambda i: (0, i)),
            pl.BlockSpec((rank, chunk), lambda i: (0, i)),
            pl.BlockSpec(summed.shape, lambda i: (0, 0)),
            pl.BlockSpec(moved.shape, lambda i: (0, 0, 0)),
        ],
        out_specs=(
            pl.BlockSpec((micro_count, tok_rows, chunk), lambda i: (0, 0, i)),
            row_spec,
            row_spec,
            row_spec,
        ),
        scratch_shapes=[
            pltpu.VMEM((tokens + 16, lanes), BF),
            pltpu.VMEM((lanes, chunk), BF),
            pltpu.VMEM((rows, 128), F32),
        ],
        name="final",
    )(spots, base, p_all, whole, own, summed, moved)


def per_device(
    activations,
    loss_grads,
    adapter_in,
    adapter_out,
    first_moment,
    second_moment,
    old_owner,
    new_owner,
    plan,
):
    sections = lax.axis_size("section")
    section_index = lax.axis_index("section")
    replicas = lax.axis_size(DP)
    my_index = lax.axis_index(DP)
    micro_count, tok_rows, width = activations.shape[1:]
    rank = adapter_in.shape[2]
    tokens = micro_count * tok_rows
    inputs = activations[0].reshape(tokens, width)
    base = loss_grads.reshape(tokens, width)
    owners_old = old_owner[0]
    owners_new = new_owner[0]
    block_len = first_moment.shape[2] // 2
    block_rows = block_len // 128
    relay_rows = block_rows // RELAYS
    replica_ids = jnp.arange(replicas, dtype=jnp.int32)

    dest = replica_ids.reshape(ND, NY, NC).transpose(2, 0, 1).reshape(-1)
    owner_match = owners_new[None, :] == jnp.concatenate([replica_ids, dest, my_index[None]])[:, None]
    inverse_all = jnp.sum(jnp.where(owner_match, replica_ids[None, :], 0), axis=1)
    inverse = inverse_all[:replicas]
    old_match = (inverse // 2)[:, None] == jnp.arange(owners_old.shape[0], dtype=jnp.int32)[None, :]
    from_row = jnp.sum(jnp.where(old_match, owners_old[None, :], 0), axis=1)
    table = jnp.stack([from_row, inverse % 2, inverse_all[replicas : 2 * replicas]])
    spots = jnp.concatenate([section_index[None], inverse_all[2 * replicas :], plan])

    turned = adapter_in[0].T
    p_all, moved, whole, summed = run_drain(
        table.astype(jnp.int32),
        inputs,
        base,
        turned,
        adapter_out[0],
        first_moment.reshape(2, RELAYS, relay_rows, 128),
        second_moment.reshape(2, RELAYS, relay_rows, 128),
    )
    emitted, update, first_next, second_next = run_final(
        spots.astype(jnp.int32),
        loss_grads,
        p_all,
        whole.reshape(sections * rank, width),
        turned,
        summed,
        moved.reshape(2, block_rows, 128),
    )
    shape = (1, 1, block_len)
    return (
        emitted[None],
        update.reshape(shape),
        first_next.reshape(shape),
        second_next.reshape(shape),
    )


def solution(mesh):
    torus = Mesh(
        mesh.devices.reshape(mesh.shape["section"], ND, NY, NC), ("section", "dp_0", "dp_1", "dp_2")
    )
    in_specs = (
        P("section", None, DP, None),
        P(None, DP, None),
        P("section", None, None),
        P("section", None, None),
        P("section", DP, None),
        P("section", DP, None),
        P("section", None),
        P("section", None),
        P(),
    )
    out_specs = (
        P("section", None, DP, None),
        P("section", DP, None),
        P("section", DP, None),
        P("section", DP, None),
    )
    return jax.shard_map(
        per_device, mesh=torus, in_specs=in_specs, out_specs=out_specs, check_vma=False
    )
```

```python
import functools

import jax
import jax.numpy as jnp
from jax import lax
from jax.experimental import pallas as pl
from jax.experimental.pallas import tpu as pltpu
from jax.sharding import Mesh
from jax.sharding import PartitionSpec as P

DP = ("dp_0", "dp_1", "dp_2")
ND, NY, NC = 4, 4, 2
SECTIONS = 8
RELAYS = 7
ALONG_Z = (1, 3, 5)
MESH = pl.DeviceIdType.MESH
BF = jnp.bfloat16
F32 = jnp.float32

beta_one = 0.9
beta_two = 0.95
adam_eps = 1e-08
adam_step = 1000.0
loss_scale = 4096.0


def dp_coords(index):
    return {"dp_0": index // (NY * NC), "dp_1": lax.rem(index // NC, NY), "dp_2": lax.rem(index, NC)}


def relay_spot(index):
    return 4 * index + index % 4


def drain_kernel(
    table_ref,
    inputs_ref,
    base_ref,
    weight_in_ref,
    weight_out_ref,
    first_ref,
    second_ref,
    emitted_ref,
    update_ref,
    next_first_ref,
    next_second_ref,
    inputs,
    base,
    pre_sum,
    act_sum,
    hidden,
    rows_got,
    packed,
    prod,
    uv_out,
    uv_got,
    total,
    moments,
    spread,
    picked,
    moved,
    whole,
    p_got,
    left,
    out,
    grad,
    flat,
    mixed_rows,
    extra_rows,
    held,
    half_out,
    half_got,
    y_out,
    y_got,
    z_out,
    z_got,
    summed,
    load_sem,
    rows_send,
    rows_recv,
    prod_send,
    prod_recv,
    uv_send,
    uv_recv,
    gather_send,
    gather_recv,
    p_send,
    p_recv,
    spread_send,
    spread_recv,
    moved_send,
    moved_recv,
    slice_send,
    slice_recv,
    wide_send,
    wide_recv,
    pair_send,
    pair_recv,
    half_send,
    half_recv,
    y_send,
    y_recv,
    z_send,
    z_recv,
    out_sem,
):
    sections = SECTIONS
    replicas = ND * NY * NC
    me = lax.axis_index("section")
    z = lax.axis_index("dp_0")
    y = lax.axis_index("dp_1")
    core = lax.axis_index("dp_2")
    dp = (z * NY + y) * NC + core
    other = 1 - core
    tokens, width = inputs.shape
    rank = weight_in_ref.shape[0]
    tok_rows = tokens // sections
    lanes = sections * rank
    parts = load_sem.shape[1]
    chunk = width // parts
    groups = chunk // 128
    block_rows = flat.shape[0] // (replicas // 2)
    half_blocks = replicas // 2
    extra = held.shape[1] - block_rows
    relay_rows = first_ref.shape[2]
    tall = rank // NY
    wide = width // NC

    def load(which, part):
        columns = pl.ds(pl.multiple_of(part * chunk, 128), chunk)
        if which == 0:
            source, target = inputs_ref.at[:, columns], inputs.at[:, columns]
        else:
            source, target = base_ref.at[:, :, columns], base.at[:, :, columns]
        return pltpu.make_async_copy(source, target, load_sem.at[which, part])

    for part in range(parts):
        load(0, part).start()
        load(1, part).start()

    barrier = pltpu.get_barrier_semaphore()
    for step in range(1, sections):
        pl.semaphore_signal(
            barrier, inc=1, device_id={"section": lax.rem(me + step, sections)}, device_id_type=MESH
        )

    def greet(step, carry):
        pl.semaphore_signal(
            barrier, inc=1, device_id=dp_coords(lax.rem(dp + step, replicas)), device_id_type=MESH
        )
        return carry

    lax.fori_loop(1, replicas, greet, 0)

    for index in range(RELAYS):
        for which, source in enumerate((first_ref, second_ref)):
            for half in range(2):
                start = (2 * which + half) * relay_rows
                moments[index, start : start + relay_rows, :] = source[half, index].astype(BF)

    for section in range(sections):

        @pl.when(section < me)
        def _(section=section):
            whole[pl.ds(section * rank, rank), :] = jnp.zeros((rank, width), BF)

        @pl.when(section == me)
        def _(section=section):
            whole[pl.ds(section * rank, rank), :] = weight_in_ref[...]

    pl.semaphore_wait(barrier, sections - 1 + replicas - 1)

    def section_copy(src, dst, send, recv, target):
        return pltpu.make_async_remote_copy(
            src_ref=src,
            dst_ref=dst,
            send_sem=send,
            recv_sem=recv,
            device_id={"section": target},
            device_id_type=MESH,
        )

    def took(view, sem):
        section_copy(view, view, sem, sem, me).wait_recv()

    def sent(view, sem):
        section_copy(view, view, sem, sem, me).wait_send()

    hop = dp // 4

    def rows_copy():
        return section_copy(
            weight_out_ref.at[pl.ds(pl.multiple_of(lax.rem(dp, 4) * tall, tall), tall)],
            rows_got,
            rows_send,
            rows_recv,
            lax.rem(me + sections - hop, sections),
        )

    @pl.when(me < hop)
    def _():
        rows_copy().start()

    def along_z(section):
        return lax.rem(section, 2) * (1 - section // 7)

    def row_of(section):
        return y + along_z(section) * (z - y)

    def slice_view(ref, section, row):
        start = pl.multiple_of(section * rank + row * tall, tall)
        return ref.at[pl.ds(start, tall), pl.ds(pl.multiple_of(core * wide, 128), wide)]

    relay = dp // 4
    is_relay = (lax.rem(dp, 4) == lax.rem(relay, 4)) & (relay < RELAYS)

    def spread_copy(index):
        peer = relay_spot(index)
        return pltpu.make_async_remote_copy(
            src_ref=moments.at[index],
            dst_ref=spread.at[dp],
            send_sem=spread_send,
            recv_sem=spread_recv,
            device_id={"dp_0": peer // 8, "dp_1": peer // 2 % 4, "dp_2": peer % 2},
            device_id_type=MESH,
        )

    across = (((1,), (1,)), ((), ()))
    down = (((0,), (0,)), ((), ()))
    pre_sum[...] = jnp.zeros_like(pre_sum)
    act_sum[...] = jnp.zeros_like(act_sum)

    def accumulate(part, carry):
        columns = pl.ds(pl.multiple_of(part * chunk, 128), chunk)
        load(0, part).wait()
        pre_sum[...] += lax.dot_general(
            inputs[:, columns], weight_in_ref[:, columns], across, preferred_element_type=F32
        )
        load(1, part).wait()
        act_sum[...] += lax.dot_general(
            base[:, :, columns].reshape(tokens, chunk),
            weight_out_ref[:, columns],
            across, preferred_element_type=F32
        )
        return carry

    lax.fori_loop(0, parts, accumulate, 0)
    pre_value = pre_sum[...]
    gate = jax.nn.sigmoid(pre_value)
    hidden[...] = (pre_value * gate).astype(BF)
    slope = gate * (1.0 + pre_value * (1.0 - gate))
    both = jnp.concatenate([act_sum[...].astype(BF), slope.astype(BF)], axis=1)
    uv_out[...] = both.reshape(sections, tok_rows, 2 * rank)

    def uv_copy(step):
        target = lax.rem(me + step, sections)
        return section_copy(uv_out.at[target], uv_got.at[me], uv_send, uv_recv, target)

    for step in range(1, sections):
        uv_copy(step).start()
    uv_got[me] = uv_out[me]

    slot = lax.rem(hop + me, sections) * 4 + lax.rem(dp, 4)
    valid = me + hop >= sections

    def prod_copy(step):
        return pltpu.make_async_remote_copy(
            src_ref=packed,
            dst_ref=prod.at[me, slot],
            send_sem=prod_send,
            recv_sem=prod_recv,
            device_id=dp_coords(lax.rem(dp + step, replicas)),
            device_id_type=MESH,
        )

    @pl.when(valid)
    def _():
        took(rows_got, rows_recv)
        piece = lax.dot_general(
            rows_got[...], weight_in_ref[...], across, preferred_element_type=F32
        )
        packed[...] = jnp.concatenate([piece[:8], piece[8:]], axis=1).astype(BF)

        def prod_start(step, carry):
            prod_copy(step).start()
            return carry

        lax.fori_loop(1, replicas, prod_start, 0)
        prod[me, slot] = packed[...]

    for section in range(1, sections):

        @pl.when(me == section)
        def _(section=section):
            row = z if section in ALONG_Z else y
            for target in reversed(range(section)):
                section_copy(
                    slice_view(weight_in_ref, 0, row),
                    slice_view(whole, section, row),
                    slice_send,
                    slice_recv.at[section],
                    target,
                ).start()

    for index in range(RELAYS):

        @pl.when(dp != relay_spot(index))
        def _(index=index):
            spread_copy(index).start()

        @pl.when(dp == relay_spot(index))
        def _(index=index):
            spread[relay_spot(index)] = moments[index]

    def outward(part, carry):
        columns = pl.ds(pl.multiple_of(part * chunk, 128), chunk)
        result = lax.dot_general(
            hidden[...],
            base[:, :, columns].reshape(tokens, chunk),
            down,
            preferred_element_type=F32,
        )
        for group in range(groups):
            flat[pl.ds(part * groups + group, rank, stride=width // 128), :] = result[
                :, group * 128 : (group + 1) * 128
            ]
        return carry

    lax.fori_loop(0, parts, outward, 0)
    for block in range(half_blocks):
        held[half_blocks + block, :block_rows] = flat[pl.ds(block * block_rows, block_rows), :]

    for section in range(1, sections):

        @pl.when((me == section) & valid)
        def _(section=section):
            took(prod.at[0, pl.ds(0, 4 * section - 1)], prod_recv)

        @pl.when((me == section) & (me + hop < sections))
        def _(section=section):
            took(prod.at[0, pl.ds(0, 4 * section)], prod_recv)

        @pl.when(me == section)
        def _(section=section):
            for step in range(1, sections):
                section_copy(
                    prod.at[section, pl.ds(0, 4 * section)],
                    prod.at[section, pl.ds(0, 4 * section)],
                    gather_send,
                    gather_recv.at[section],
                    (section - step) % sections,
                ).start()

    def wide_copy(section, shift):
        view = slice_view(whole, section, row_of(section))
        axis, at, count = ("dp_0", z, ND) if section in ALONG_Z else ("dp_1", y, NY)
        return pltpu.make_async_remote_copy(
            src_ref=view,
            dst_ref=view,
            send_sem=wide_send.at[section],
            recv_sem=wide_recv.at[section],
            device_id={axis: lax.rem(at + shift, count)},
            device_id_type=MESH,
        )

    def spread_adapters(chosen):
        for section in chosen:

            @pl.when(me < section)
            def _(section=section):
                took(slice_view(whole, section, row_of(section)), slice_recv.at[section])
                for shift in (1, 3, 2):
                    wide_copy(section, shift).start()

    spread_adapters([section for section in range(1, sections) if section not in ALONG_Z])

    def moved_copy(step):
        peer = lax.rem(dp + step, replicas)
        return pltpu.make_async_remote_copy(
            src_ref=picked.at[peer],
            dst_ref=moved.at[relay],
            send_sem=moved_send,
            recv_sem=moved_recv,
            device_id=dp_coords(peer),
            device_id_type=MESH,
        )

    took(uv_got.at[pl.ds(0, sections - 1)], uv_recv)
    for section in range(1, sections):

        @pl.when(me != section)
        def _(section=section):
            took(prod.at[section, pl.ds(0, 4 * section)], gather_recv.at[section])

    total[...] = jnp.zeros_like(total)
    for turn in reversed(range(sections)):
        low, high = turn * rank, (turn + 1) * rank
        pair = uv_got[turn].astype(F32)
        p_value = ((pair[:, :rank] + total[:, low:high]) * pair[:, rank:]).astype(BF)
        p_got[me, :, low:high] = p_value
        if turn:
            got = prod[turn, : 4 * turn].astype(F32)
            rows = jnp.concatenate([got[:, :, :rank], got[:, :, rank:]], axis=1)
            rows = rows.reshape(turn * rank, rank).astype(BF)
            total[:, :low] += lax.dot_general(p_value, rows, across, preferred_element_type=F32)

    def live(section):
        start = section // 2 * 2 * rank
        return pl.ds(start, lanes - start)

    def p_copy(section):
        view = p_got.at[me, :, live(section)]
        return section_copy(view, view, p_send.at[section], p_recv, section)

    for section in range(sections):

        @pl.when(me != section)
        def _(section=section):
            p_copy(section).start()

    spread_adapters(ALONG_Z)

    @pl.when(is_relay)
    def _():
        took(spread.at[pl.ds(0, replicas - 1)], spread_recv)

        def pick(target, carry):
            rows = spread[table_ref[0, target]].astype(F32)
            upper = table_ref[1, target] > 0
            for which in range(2):
                start = 2 * which * relay_rows
                low = rows[start : start + relay_rows]
                high = rows[start + relay_rows : start + 2 * relay_rows]
                picked[target, which * relay_rows : (which + 1) * relay_rows, :] = jnp.where(
                    upper, high, low
                ).astype(BF)
            return carry

        lax.fori_loop(0, replicas, pick, 0)

        def moved_start(step, carry):
            moved_copy(step).start()
            return carry

        lax.fori_loop(1, replicas, moved_start, 0)
        moved[relay] = picked[dp]

    for section in range(sections):

        @pl.when(me == section)
        def _(section=section):
            took(p_got.at[pl.ds(0, sections - 1), :, live(section)], p_recv)

    lane_section = lax.broadcasted_iota(jnp.int32, (tokens, lanes), 1) // rank
    p_all = p_got[...].reshape(tokens, lanes)
    p_above = jnp.where(lane_section > me, p_all, jnp.zeros_like(p_all))
    p_live = jnp.where(lane_section == me, p_all, jnp.zeros_like(p_all))
    take = lax.rem(lax.broadcasted_iota(jnp.int32, (lanes, rank), 0), rank) == (
        lax.broadcasted_iota(jnp.int32, (lanes, rank), 1)
    )
    p_mine = jnp.dot(p_live, take.astype(F32).astype(BF), preferred_element_type=F32).astype(BF)

    def inward(part, carry):
        columns = pl.ds(pl.multiple_of(part * chunk, 128), chunk)
        grad[columns, :] = lax.dot_general(
            inputs[:, columns], p_mine, down, preferred_element_type=F32
        )
        return carry

    lax.fori_loop(0, parts, inward, 0)
    mixed = lax.dot_general(hidden[...], p_above, down, preferred_element_type=F32)
    for group in range(lanes // 128):
        mixed_rows[pl.ds(group, rank, stride=lanes // 128), :] = mixed[
            :, group * 128 : (group + 1) * 128
        ]
    for block in range(half_blocks):
        even = grad[pl.ds(block * 2 * block_rows, block_rows, stride=2), :]
        odd = grad[pl.ds(block * 2 * block_rows + 1, block_rows, stride=2), :]
        held[block, :block_rows] = jnp.concatenate([even, odd], axis=1)
        held[block, block_rows:] = jnp.zeros((extra, 128), F32)
        held[half_blocks + block, block_rows:] = mixed_rows[pl.ds(block * extra, extra), :]

    order = (2, 1, 3, 0)

    def half_copy(far):
        return pltpu.make_async_remote_copy(
            src_ref=half_out.at[far],
            dst_ref=half_got.at[far],
            send_sem=half_send.at[far],
            recv_sem=half_recv.at[far],
            device_id={"dp_2": other},
            device_id_type=MESH,
        )

    def y_copy(far, step):
        there = lax.rem(y + step, NY)
        return pltpu.make_async_remote_copy(
            src_ref=y_out.at[far, there],
            dst_ref=y_got.at[far, step],
            send_sem=y_send.at[far],
            recv_sem=y_recv.at[far],
            device_id={"dp_1": there},
            device_id_type=MESH,
        )

    def z_copy(far):
        return pltpu.make_async_remote_copy(
            src_ref=z_out.at[far],
            dst_ref=z_got.at[far],
            send_sem=z_send.at[far],
            recv_sem=z_recv.at[far],
            device_id={"dp_0": lax.rem(z + far, ND)},
            device_id_type=MESH,
        )

    for far in order:
        there = lax.rem(z + far, ND)
        for column in range(NY):
            half_out[far, column] = held[table_ref[2, (other * ND + there) * NY + column]].astype(BF)
        half_copy(far).start()
    for far in order:
        there = lax.rem(z + far, ND)
        half_copy(far).wait_recv()
        for column in range(NY):
            own = held[table_ref[2, (core * ND + there) * NY + column]]
            y_out[far, column] = (own + half_got[far, column].astype(F32)).astype(BF)
        for step in (2, 1, 3):
            y_copy(far, step).start()
    def pair_copy(section):
        view = whole.at[
            pl.ds(section * rank, rank), pl.ds(pl.multiple_of(core * wide, 128), wide)
        ]
        return pltpu.make_async_remote_copy(
            src_ref=view,
            dst_ref=view,
            send_sem=pair_send.at[section],
            recv_sem=pair_recv.at[section],
            device_id={"dp_2": other},
            device_id_type=MESH,
        )

    place = lax.broadcasted_iota(jnp.int32, (tok_rows, lanes), 1) // rank
    for micro in range(sections):
        value = p_got[table_ref[3, micro]]
        left[micro * tok_rows : (micro + 1) * tok_rows, :] = jnp.where(
            place >= me, value, jnp.zeros_like(value)
        )

    for section in range(1, sections):

        @pl.when(me < section)
        def _(section=section):
            took(
                whole.at[pl.ds(section * rank, 3 * tall), pl.ds(0, wide)], wide_recv.at[section]
            )
            pair_copy(section).start()

    for far in order:
        took(y_got.at[far, pl.ds(1, NY - 1)], y_recv.at[far])
        part = y_out[far, y].astype(F32)
        for step in range(1, NY):
            part += y_got[far, step].astype(F32)
        if far:
            z_out[far] = part.astype(BF)
            z_copy(far).start()
        else:
            summed[...] = part

    for section in range(1, sections):

        @pl.when(me < section)
        def _(section=section):
            pair_copy(section).wait_recv()

    slabs = out_sem.shape[0]
    slab = width // slabs

    def out_copy(index):
        columns = pl.ds(pl.multiple_of(index * slab, 128), slab)
        return pltpu.make_async_copy(
            out.at[:, :, columns], emitted_ref.at[:, :, columns], out_sem.at[index]
        )

    def emit(index, carry):
        columns = pl.ds(pl.multiple_of(index * slab, 128), slab)
        result = jnp.dot(left[...], whole[:, columns], preferred_element_type=F32)
        for micro in range(sections):
            added = result[micro * tok_rows : (micro + 1) * tok_rows]
            out[micro, :, columns] = (
                base[table_ref[3, micro], :, columns].astype(F32) + added
            ).astype(BF)
        out_copy(index).start()
        return carry

    lax.fori_loop(0, slabs, emit, 0)

    for far in range(1, ND):
        z_copy(far).wait_recv()
    result = summed[...]
    for far in range(1, ND):
        result += z_got[far].astype(F32)
    summed[...] = result

    apart = lanes // 128
    mixed = jnp.concatenate(
        [summed[pl.ds(block_rows + group, 4, stride=apart), :] for group in range(apart)], axis=1
    )
    mixed = jnp.concatenate([mixed, jnp.zeros((12, lanes), F32)], axis=0).astype(BF)

    def correct(index, carry):
        columns = pl.ds(pl.multiple_of(index * slab, 128), slab)
        result = jnp.dot(mixed, whole[:, columns], preferred_element_type=F32)
        for group in range(slab // 128):
            extra_rows[pl.ds(index * (slab // 128) + group, 4, stride=width // 128), :] = result[
                :4, group * 128 : (group + 1) * 128
            ]
        return carry

    lax.fori_loop(0, slabs, correct, 0)

    @pl.when(is_relay)
    def _():
        took(moved.at[pl.ds(0, RELAYS - 1)], moved_recv)
        sent(picked.at[pl.ds(0, replicas - 1)], moved_send)
        sent(spread.at[pl.ds(0, RELAYS - 1)], spread_send)

    @pl.when(jnp.logical_not(is_relay))
    def _():
        took(moved, moved_recv)
        sent(spread.at[pl.ds(0, RELAYS)], spread_send)

    is_out = table_ref[4, 0] >= half_blocks
    main = summed[:block_rows, :]
    grads = jnp.where(is_out, main + extra_rows[...], main) / loss_scale
    for index in range(RELAYS):
        at = slice(index * relay_rows, (index + 1) * relay_rows)
        old = moved[index].astype(F32)
        g = grads[at]
        first_next = beta_one * old[:relay_rows] + (1.0 - beta_one) * g
        second_next = beta_two * old[relay_rows:] + (1.0 - beta_two) * g * g
        next_first_ref[at, :] = first_next
        next_second_ref[at, :] = second_next
        update_ref[at, :] = (
            first_next
            / (1.0 - beta_one**adam_step)
            / (jnp.sqrt(second_next / (1.0 - beta_two**adam_step)) + adam_eps)
        )

    @pl.when(me < hop)
    def _():
        rows_copy().wait_send()

    @pl.when(valid)
    def _():
        sent(prod.at[0, pl.ds(0, replicas - 1)], prod_send)

    sent(uv_out.at[pl.ds(0, sections - 1)], uv_send)
    for section in range(sections):

        @pl.when(me != section)
        def _(section=section):
            p_copy(section).wait_send()

    for section in range(1, sections):

        @pl.when(me == section)
        def _(section=section):
            sent(prod.at[pl.ds(0, sections - 1), pl.ds(0, 4 * section)], gather_send)
            sent(whole.at[pl.ds(0, section * tall), pl.ds(0, wide)], slice_send)

        @pl.when(me < section)
        def _(section=section):
            sent(whole.at[pl.ds(0, 3 * tall), pl.ds(0, wide)], wide_send.at[section])
            pair_copy(section).wait_send()

    for far in range(ND):
        half_copy(far).wait_send()
        sent(y_got.at[far, pl.ds(1, NY - 1)], y_send.at[far])
        if far:
            z_copy(far).wait_send()

    for index in range(slabs):
        out_copy(index).wait()


def vmem():
    return pl.BlockSpec(memory_space=pltpu.VMEM)


def smem():
    return pl.BlockSpec(memory_space=pltpu.SMEM)


def hbm():
    return pl.BlockSpec(memory_space=pl.ANY)


def run_drain(table, inputs, base, turned, weight_out, first, second):
    tokens, width = inputs.shape
    rank = turned.shape[0]
    sections = SECTIONS
    replicas = ND * NY * NC
    tok_rows = tokens // sections
    lanes = sections * rank
    half_blocks = replicas // 2
    rows = width * rank // half_blocks // 128
    extra = rank * lanes // 128 // half_blocks
    relay_rows = first.shape[2]
    dma = pltpu.SemaphoreType.DMA
    full = (rows + extra, 128)
    per_section = dma((sections,))
    per_z = dma((ND,))
    row_shape = jax.ShapeDtypeStruct((rows, 128), F32)
    return pl.pallas_call(
        drain_kernel,
        out_shape=(
            jax.ShapeDtypeStruct((sections, tok_rows, width), BF),
            row_shape,
            row_shape,
            row_shape,
        ),
        in_specs=[smem()] + [hbm()] * 2 + [vmem()] * 4,
        out_specs=(hbm(), vmem(), vmem(), vmem()),
        scratch_shapes=[
            pltpu.VMEM((tokens, width), BF),
            pltpu.VMEM((sections, tok_rows, width), BF),
            pltpu.VMEM((tokens, rank), F32),
            pltpu.VMEM((tokens, rank), F32),
            pltpu.VMEM((tokens, rank), BF),
            pltpu.VMEM((rank // NY, width), BF),
            pltpu.VMEM((8, 128), BF),
            pltpu.VMEM((sections, 32, 8, 128), BF),
            pltpu.VMEM((sections, tok_rows, 2 * rank), BF),
            pltpu.VMEM((sections, tok_rows, 2 * rank), BF),
            pltpu.VMEM((tok_rows, lanes), F32),
            pltpu.VMEM((RELAYS, 4 * relay_rows, 128), BF),
            pltpu.VMEM((replicas, 4 * relay_rows, 128), BF),
            pltpu.VMEM((replicas, 2 * relay_rows, 128), BF),
            pltpu.VMEM((RELAYS, 2 * relay_rows, 128), BF),
            pltpu.VMEM((lanes, width), BF),
            pltpu.VMEM((sections, tok_rows, lanes), BF),
            pltpu.VMEM((tokens, lanes), BF),
            pltpu.VMEM((sections, tok_rows, width), BF),
            pltpu.VMEM((width, rank), F32),
            pltpu.VMEM((half_blocks * rows, 128), F32),
            pltpu.VMEM((half_blocks * extra, 128), F32),
            pltpu.VMEM((rows, 128), F32),
            pltpu.VMEM((replicas, *full), F32),
            pltpu.VMEM((ND, NY, *full), BF),
            pltpu.VMEM((ND, NY, *full), BF),
            pltpu.VMEM((ND, NY, *full), BF),
            pltpu.VMEM((ND, NY, *full), BF),
            pltpu.VMEM((ND, *full), BF),
            pltpu.VMEM((ND, *full), BF),
            pltpu.VMEM(full, F32),
            dma((2, 6)),
            dma,
            dma,
            dma,
            dma,
            dma,
            dma,
            dma,
            per_section,
            per_section,
            dma,
            dma,
            dma,
            dma,
            dma,
            dma,
            per_section,
            per_section,
            per_section,
            per_section,
            per_section,
            per_z,
            per_z,
            per_z,
            per_z,
            per_z,
            per_z,
            dma((7,)),
        ],
        compiler_params=pltpu.CompilerParams(
            collective_id=0, has_side_effects=True, vmem_limit_bytes=60 * 2**20
        ),
        name="drain",
    )(table, inputs, base, turned, weight_out, first, second)


def per_device(
    activations,
    loss_grads,
    adapter_in,
    adapter_out,
    first_moment,
    second_moment,
    old_owner,
    new_owner,
    plan,
):
    replicas = lax.axis_size(DP)
    my_index = lax.axis_index(DP)
    micro_count, tok_rows, width = activations.shape[1:]
    rank = adapter_in.shape[2]
    tokens = micro_count * tok_rows
    inputs = activations[0].reshape(tokens, width)
    owners_old = old_owner[0]
    owners_new = new_owner[0]
    block_len = first_moment.shape[2] // 2
    block_rows = block_len // 128
    relay_rows = block_rows // RELAYS
    replica_ids = jnp.arange(replicas, dtype=jnp.int32)

    dest = replica_ids.reshape(ND, NY, NC).transpose(2, 0, 1).reshape(-1)
    owner_match = owners_new[None, :] == jnp.concatenate([replica_ids, dest, my_index[None]])[:, None]
    inverse_all = jnp.sum(jnp.where(owner_match, replica_ids[None, :], 0), axis=1)
    inverse = inverse_all[:replicas]
    old_match = (inverse // 2)[:, None] == jnp.arange(owners_old.shape[0], dtype=jnp.int32)[None, :]
    from_row = jnp.sum(jnp.where(old_match, owners_old[None, :], 0), axis=1)
    padded = jnp.concatenate([plan, jnp.zeros((replicas - micro_count,), jnp.int32)])
    my_block = jnp.broadcast_to(inverse_all[2 * replicas :], (replicas,))
    table = jnp.stack(
        [from_row, inverse % 2, inverse_all[replicas : 2 * replicas], padded, my_block]
    )
    emitted, update, first_next, second_next = run_drain(
        table.astype(jnp.int32),
        inputs,
        loss_grads,
        adapter_in[0].T,
        adapter_out[0],
        first_moment.reshape(2, RELAYS, relay_rows, 128),
        second_moment.reshape(2, RELAYS, relay_rows, 128),
    )
    shape = (1, 1, block_len)
    return (
        emitted[None],
        update.reshape(shape),
        first_next.reshape(shape),
        second_next.reshape(shape),
    )


def solution(mesh):
    torus = Mesh(
        mesh.devices.reshape(mesh.shape["section"], ND, NY, NC), ("section", "dp_0", "dp_1", "dp_2")
    )
    in_specs = (
        P("section", None, DP, None),
        P(None, DP, None),
        P("section", None, None),
        P("section", None, None),
        P("section", DP, None),
        P("section", DP, None),
        P("section", None),
        P("section", None),
        P(),
    )
    out_specs = (
        P("section", None, DP, None),
        P("section", DP, None),
        P("section", DP, None),
        P("section", DP, None),
    )
    return jax.shard_map(
        per_device, mesh=torus, in_specs=in_specs, out_specs=out_specs, check_vma=False
    )
```

```python
import functools

import jax
import jax.numpy as jnp
from jax import lax
from jax.experimental import pallas as pl
from jax.experimental.pallas import tpu as pltpu
from jax.sharding import Mesh
from jax.sharding import PartitionSpec as P

DP = ("dp_0", "dp_1", "dp_2")
ND, NY, NC = 4, 4, 2
SECTIONS = 8
RELAYS = 7
ALONG_Z = (1, 2,)
MESH = pl.DeviceIdType.MESH
BF = jnp.bfloat16
F32 = jnp.float32

beta_one = 0.9
beta_two = 0.95
adam_eps = 1e-08
adam_step = 1000.0
loss_scale = 4096.0


def dp_coords(index):
    return {"dp_0": index // (NY * NC), "dp_1": lax.rem(index // NC, NY), "dp_2": lax.rem(index, NC)}


def relay_spot(index):
    return 4 * index + index % 4


def drain_kernel(
    table_ref,
    old_ref,
    plan_ref,
    inputs_ref,
    base_ref,
    weight_in_ref,
    weight_out_ref,
    first_ref,
    second_ref,
    out,
    grads_ref,
    moved,
    inputs,
    base,
    pre_sum,
    act_sum,
    hidden,
    rows_got,
    packed,
    prod,
    uv_out,
    uv_got,
    total,
    moments,
    spread,
    picked,
    whole,
    p_got,
    left,
    grad,
    flat,
    mixed_rows,
    extra_rows,
    held,
    half_out,
    half_got,
    y_out,
    y_got,
    z_out,
    z_got,
    summed,
    load_sem,
    rows_send,
    rows_recv,
    prod_send,
    prod_recv,
    uv_send,
    uv_recv,
    gather_send,
    gather_recv,
    p_send,
    p_recv,
    spread_send,
    spread_recv,
    moved_send,
    moved_recv,
    slice_send,
    slice_recv,
    pass_send,
    wide_send,
    wide_recv,
    pair_send,
    pair_recv,
    half_send,
    half_recv,
    y_send,
    y_recv,
    z_send,
    z_recv,
):
    sections = SECTIONS
    replicas = ND * NY * NC
    me = lax.axis_index("section")
    z = lax.axis_index("dp_0")
    y = lax.axis_index("dp_1")
    core = lax.axis_index("dp_2")
    dp = (z * NY + y) * NC + core
    other = 1 - core
    tokens, width = inputs.shape
    rank = weight_in_ref.shape[0]
    tok_rows = tokens // sections
    lanes = sections * rank
    parts = load_sem.shape[1]
    chunk = width // parts
    groups = chunk // 128
    block_rows = flat.shape[0] // (replicas // 2)
    half_blocks = replicas // 2
    extra = held.shape[1] - block_rows
    relay_rows = first_ref.shape[2]
    tall = rank // NY
    wide = width // NC

    def load(which, part):
        columns = pl.ds(pl.multiple_of(part * chunk, 128), chunk)
        if which == 0:
            source, target = inputs_ref.at[:, columns], inputs.at[:, columns]
        else:
            source, target = base_ref.at[:, :, columns], base.at[:, :, columns]
        return pltpu.make_async_copy(source, target, load_sem.at[which, part])

    for part in range(parts):
        load(0, part).start()
        load(1, part).start()

    barrier = pltpu.get_barrier_semaphore()
    for step in range(1, sections):
        pl.semaphore_signal(
            barrier, inc=1, device_id={"section": lax.rem(me + step, sections)}, device_id_type=MESH
        )

    def greet(step, carry):
        pl.semaphore_signal(
            barrier, inc=1, device_id=dp_coords(lax.rem(dp + step, replicas)), device_id_type=MESH
        )
        return carry

    lax.fori_loop(1, replicas, greet, 0)

    for index in range(RELAYS):
        for which, source in enumerate((first_ref, second_ref)):
            for half in range(2):
                start = (2 * which + half) * relay_rows
                moments[index, start : start + relay_rows, :] = source[half, index].astype(BF)

    for section in range(sections):

        @pl.when(section < me)
        def _(section=section):
            whole[pl.ds(section * rank, rank), :] = jnp.zeros((rank, width), BF)

        @pl.when(section == me)
        def _(section=section):
            whole[pl.ds(section * rank, rank), :] = weight_in_ref[...]

    pl.semaphore_wait(barrier, sections - 1 + replicas - 1)

    def section_copy(src, dst, send, recv, target):
        return pltpu.make_async_remote_copy(
            src_ref=src,
            dst_ref=dst,
            send_sem=send,
            recv_sem=recv,
            device_id={"section": target},
            device_id_type=MESH,
        )

    def took(view, sem):
        section_copy(view, view, sem, sem, me).wait_recv()

    def sent(view, sem):
        section_copy(view, view, sem, sem, me).wait_send()

    hop = dp // 4

    def rows_copy():
        return section_copy(
            weight_out_ref.at[pl.ds(pl.multiple_of(lax.rem(dp, 4) * tall, tall), tall)],
            rows_got,
            rows_send,
            rows_recv,
            lax.rem(me + sections - hop, sections),
        )

    def slice_view(ref, section, row):
        start = pl.multiple_of(section * rank + row * tall, tall)
        return ref.at[pl.ds(start, tall), pl.ds(pl.multiple_of(core * wide, 128), wide)]

    @pl.when(me < hop)
    def _():
        rows_copy().start()

    half = sections // 2

    def slice_copy(source, section, send, target):
        row = z if section in ALONG_Z else y
        start = 0 if source is weight_in_ref else section
        return section_copy(
            slice_view(source, start, row),
            slice_view(whole, section, row),
            send,
            slice_recv.at[section],
            target,
        )

    def slice_targets(section):
        first = section // half * half
        return [section - half] * (section >= half) + list(range(first, section))

    for section in range(1, sections):

        @pl.when(me == section)
        def _(section=section):
            for target in slice_targets(section):
                slice_copy(weight_in_ref, section, slice_send, target).start()

    def row_of(section):
        return z if section in ALONG_Z else y

    relay = dp // 4
    is_relay = (lax.rem(dp, 4) == lax.rem(relay, 4)) & (relay < RELAYS)

    def spread_copy(index):
        peer = relay_spot(index)
        return pltpu.make_async_remote_copy(
            src_ref=moments.at[index],
            dst_ref=spread.at[dp],
            send_sem=spread_send,
            recv_sem=spread_recv,
            device_id={"dp_0": peer // 8, "dp_1": peer // 2 % 4, "dp_2": peer % 2},
            device_id_type=MESH,
        )

    across = (((1,), (1,)), ((), ()))
    down = (((0,), (0,)), ((), ()))
    pre_sum[...] = jnp.zeros_like(pre_sum)
    act_sum[...] = jnp.zeros_like(act_sum)

    def accumulate(part, carry):
        columns = pl.ds(pl.multiple_of(part * chunk, 128), chunk)
        load(0, part).wait()
        pre_sum[...] += lax.dot_general(
            inputs[:, columns], weight_in_ref[:, columns], across, preferred_element_type=F32
        )
        load(1, part).wait()
        act_sum[...] += lax.dot_general(
            base[:, :, columns].reshape(tokens, chunk),
            weight_out_ref[:, columns],
            across, preferred_element_type=F32
        )
        return carry

    lax.fori_loop(0, parts, accumulate, 0)
    for section in range(half):

        @pl.when(me == section)
        def _(section=section):
            above = section + half
            took(slice_view(whole, above, row_of(above)), slice_recv.at[above])
            for step in (1, 3, 2):
                slice_copy(whole, above, pass_send, (section + step) % half).start()

    pre_value = pre_sum[...]
    gate = jax.nn.sigmoid(pre_value)
    hidden[...] = (pre_value * gate).astype(BF)
    slope = gate * (1.0 + pre_value * (1.0 - gate))
    both = jnp.concatenate([act_sum[...].astype(BF), slope.astype(BF)], axis=1)
    uv_out[...] = both.reshape(sections, tok_rows, 2 * rank)

    def uv_copy(step):
        target = lax.rem(me + step, sections)
        return section_copy(uv_out.at[target], uv_got.at[me], uv_send, uv_recv, target)

    for step in range(1, sections):
        uv_copy(step).start()
    uv_got[me] = uv_out[me]

    slot = lax.rem(hop + me, sections) * 4 + lax.rem(dp, 4)
    valid = me + hop >= sections

    def prod_copy(step):
        return pltpu.make_async_remote_copy(
            src_ref=packed,
            dst_ref=prod.at[me, slot],
            send_sem=prod_send,
            recv_sem=prod_recv,
            device_id=dp_coords(lax.rem(dp + step, replicas)),
            device_id_type=MESH,
        )

    @pl.when(valid)
    def _():
        took(rows_got, rows_recv)
        piece = lax.dot_general(
            rows_got[...], weight_in_ref[...], across, preferred_element_type=F32
        )
        packed[...] = jnp.concatenate([piece[:8], piece[8:]], axis=1).astype(BF)

        def prod_start(step, carry):
            prod_copy(step).start()
            return carry

        lax.fori_loop(1, replicas, prod_start, 0)
        prod[me, slot] = packed[...]

    def outward(part, carry):
        columns = pl.ds(pl.multiple_of(part * chunk, 128), chunk)
        result = lax.dot_general(
            hidden[...],
            base[:, :, columns].reshape(tokens, chunk),
            down,
            preferred_element_type=F32,
        )
        for group in range(groups):
            flat[pl.ds(part * groups + group, rank, stride=width // 128), :] = result[
                :, group * 128 : (group + 1) * 128
            ]
        return carry

    lax.fori_loop(0, parts, outward, 0)
    for block in range(half_blocks):
        held[half_blocks + block, :block_rows] = flat[pl.ds(block * block_rows, block_rows), :]

    for section in range(1, sections):

        @pl.when((me == section) & valid)
        def _(section=section):
            took(prod.at[0, pl.ds(0, 4 * section - 1)], prod_recv)

        @pl.when((me == section) & (me + hop < sections))
        def _(section=section):
            took(prod.at[0, pl.ds(0, 4 * section)], prod_recv)

        @pl.when(me == section)
        def _(section=section):
            for step in range(1, sections):
                section_copy(
                    prod.at[section, pl.ds(0, 4 * section)],
                    prod.at[section, pl.ds(0, 4 * section)],
                    gather_send,
                    gather_recv.at[section],
                    (section - step) % sections,
                ).start()

    def wide_copy(section, shift):
        view = slice_view(whole, section, row_of(section))
        axis, at, count = ("dp_0", z, ND) if section in ALONG_Z else ("dp_1", y, NY)
        return pltpu.make_async_remote_copy(
            src_ref=view,
            dst_ref=view,
            send_sem=wide_send.at[section],
            recv_sem=wide_recv.at[section],
            device_id={axis: lax.rem(at + shift, count)},
            device_id_type=MESH,
        )

    def spread_adapters(chosen):
        for section in chosen:

            @pl.when(me < section)
            def _(section=section):
                @pl.when((me >= half) | (me + half != section))
                def _():
                    took(slice_view(whole, section, row_of(section)), slice_recv.at[section])

                for shift in (1, 3, 2):
                    wide_copy(section, shift).start()

    def moved_copy(step):
        peer = lax.rem(dp + step, replicas)
        return pltpu.make_async_remote_copy(
            src_ref=picked.at[peer],
            dst_ref=moved.at[relay],
            send_sem=moved_send,
            recv_sem=moved_recv,
            device_id=dp_coords(peer),
            device_id_type=MESH,
        )

    for index in range(RELAYS):

        @pl.when(dp != relay_spot(index))
        def _(index=index):
            spread_copy(index).start()

        @pl.when(dp == relay_spot(index))
        def _(index=index):
            spread[relay_spot(index)] = moments[index]

    spread_adapters([section for section in range(1, sections) if section not in ALONG_Z])
    took(uv_got.at[pl.ds(0, sections - 1)], uv_recv)
    for section in range(1, sections):

        @pl.when(me != section)
        def _(section=section):
            took(prod.at[section, pl.ds(0, 4 * section)], gather_recv.at[section])

    total[...] = jnp.zeros_like(total)
    for turn in reversed(range(sections)):
        low, high = turn * rank, (turn + 1) * rank
        pair = uv_got[turn].astype(F32)
        p_value = ((pair[:, :rank] + total[:, low:high]) * pair[:, rank:]).astype(BF)
        p_got[me, :, low:high] = p_value
        if turn:
            got = prod[turn, : 4 * turn].astype(F32)
            rows = jnp.concatenate([got[:, :, :rank], got[:, :, rank:]], axis=1)
            rows = rows.reshape(turn * rank, rank).astype(BF)
            total[:, :low] += lax.dot_general(p_value, rows, across, preferred_element_type=F32)

    def live(section):
        start = section // 2 * 2 * rank
        return pl.ds(start, lanes - start)

    def p_copy(section):
        view = p_got.at[me, :, live(section)]
        return section_copy(view, view, p_send.at[section], p_recv, section)

    for section in range(sections):

        @pl.when(me != section)
        def _(section=section):
            p_copy(section).start()

    spread_adapters(ALONG_Z)

    for section in range(sections):

        @pl.when(me == section)
        def _(section=section):
            took(p_got.at[pl.ds(0, sections - 1), :, live(section)], p_recv)

    lane_section = lax.broadcasted_iota(jnp.int32, (tokens, lanes), 1) // rank
    p_all = p_got[...].reshape(tokens, lanes)
    p_above = jnp.where(lane_section > me, p_all, jnp.zeros_like(p_all))
    p_live = jnp.where(lane_section == me, p_all, jnp.zeros_like(p_all))
    take = lax.rem(lax.broadcasted_iota(jnp.int32, (lanes, rank), 0), rank) == (
        lax.broadcasted_iota(jnp.int32, (lanes, rank), 1)
    )
    p_mine = jnp.dot(p_live, take.astype(F32).astype(BF), preferred_element_type=F32).astype(BF)

    def inward(part, carry):
        columns = pl.ds(pl.multiple_of(part * chunk, 128), chunk)
        grad[columns, :] = lax.dot_general(
            inputs[:, columns], p_mine, down, preferred_element_type=F32
        )
        return carry

    lax.fori_loop(0, parts, inward, 0)
    mixed = lax.dot_general(hidden[...], p_above, down, preferred_element_type=F32)
    for group in range(lanes // 128):
        mixed_rows[pl.ds(group, rank, stride=lanes // 128), :] = mixed[
            :, group * 128 : (group + 1) * 128
        ]
    for block in range(half_blocks):
        even = grad[pl.ds(block * 2 * block_rows, block_rows, stride=2), :]
        odd = grad[pl.ds(block * 2 * block_rows + 1, block_rows, stride=2), :]
        held[block, :block_rows] = jnp.concatenate([even, odd], axis=1)
        held[block, block_rows:] = jnp.zeros((extra, 128), F32)
        held[half_blocks + block, block_rows:] = mixed_rows[pl.ds(block * extra, extra), :]

    order = (2, 1, 3, 0)

    def half_copy(far):
        return pltpu.make_async_remote_copy(
            src_ref=half_out.at[far],
            dst_ref=half_got.at[far],
            send_sem=half_send.at[far],
            recv_sem=half_recv.at[far],
            device_id={"dp_2": other},
            device_id_type=MESH,
        )

    def y_copy(far, step):
        there = lax.rem(y + step, NY)
        return pltpu.make_async_remote_copy(
            src_ref=y_out.at[far, there],
            dst_ref=y_got.at[far, step],
            send_sem=y_send.at[far],
            recv_sem=y_recv.at[far],
            device_id={"dp_1": there},
            device_id_type=MESH,
        )

    def z_copy(far):
        return pltpu.make_async_remote_copy(
            src_ref=z_out.at[far],
            dst_ref=z_got.at[far],
            send_sem=z_send.at[far],
            recv_sem=z_recv.at[far],
            device_id={"dp_0": lax.rem(z + far, ND)},
            device_id_type=MESH,
        )

    for far in order:
        there = lax.rem(z + far, ND)
        for column in range(NY):
            half_out[far, column] = held[table_ref[(there * NY + column) * NC + other]].astype(BF)
        half_copy(far).start()
    for far in order:
        there = lax.rem(z + far, ND)
        half_copy(far).wait_recv()
        for column in range(NY):
            own = held[table_ref[(there * NY + column) * NC + core]]
            y_out[far, column] = (own + half_got[far, column].astype(F32)).astype(BF)
        for step in (2, 1, 3):
            y_copy(far, step).start()
    def pair_copy(section):
        view = whole.at[
            pl.ds(section * rank, rank), pl.ds(pl.multiple_of(core * wide, 128), wide)
        ]
        return pltpu.make_async_remote_copy(
            src_ref=view,
            dst_ref=view,
            send_sem=pair_send.at[section],
            recv_sem=pair_recv.at[section],
            device_id={"dp_2": other},
            device_id_type=MESH,
        )

    place = lax.broadcasted_iota(jnp.int32, (tok_rows, lanes), 1) // rank
    for micro in range(sections):
        value = p_got[plan_ref[micro]]
        left[micro * tok_rows : (micro + 1) * tok_rows, :] = jnp.where(
            place >= me, value, jnp.zeros_like(value)
        )

    @pl.when(is_relay)
    def _():
        took(spread.at[pl.ds(0, replicas - 1)], spread_recv)

        def pick(target, carry):
            rows = spread[old_ref[table_ref[target] // 2]].astype(F32)
            upper = lax.rem(table_ref[target], 2) > 0
            for which in range(2):
                start = 2 * which * relay_rows
                low = rows[start : start + relay_rows]
                high = rows[start + relay_rows : start + 2 * relay_rows]
                picked[target, which * relay_rows : (which + 1) * relay_rows, :] = jnp.where(
                    upper, high, low
                ).astype(BF)
            return carry

        lax.fori_loop(0, replicas, pick, 0)

        def moved_start(step, carry):
            moved_copy(step).start()
            return carry

        lax.fori_loop(1, replicas, moved_start, 0)
        moved[relay] = picked[dp]

    for section in range(1, sections):

        @pl.when(me < section)
        def _(section=section):
            took(
                whole.at[pl.ds(section * rank, 3 * tall), pl.ds(0, wide)], wide_recv.at[section]
            )
            pair_copy(section).start()

    for far in order:
        took(y_got.at[far, pl.ds(1, NY - 1)], y_recv.at[far])
        part = y_out[far, y].astype(F32)
        for step in range(1, NY):
            part += y_got[far, step].astype(F32)
        if far:
            z_out[far] = part.astype(BF)
            z_copy(far).start()
        else:
            summed[...] = part

    for section in range(1, sections):

        @pl.when(me < section)
        def _(section=section):
            pair_copy(section).wait_recv()

    slabs = 7
    slab = width // slabs

    def emit(index, carry):
        columns = pl.ds(pl.multiple_of(index * slab, 128), slab)
        result = jnp.dot(left[...], whole[:, columns], preferred_element_type=F32)
        for micro in range(sections):
            added = result[micro * tok_rows : (micro + 1) * tok_rows]
            out[micro, :, columns] = (
                base[plan_ref[micro], :, columns].astype(F32) + added
            ).astype(BF)
        return carry

    lax.fori_loop(0, slabs, emit, 0)

    for far in range(1, ND):
        z_copy(far).wait_recv()
    result = summed[...]
    for far in range(1, ND):
        result += z_got[far].astype(F32)
    summed[...] = result

    apart = lanes // 128
    mixed = jnp.concatenate(
        [summed[pl.ds(block_rows + group, 4, stride=apart), :] for group in range(apart)], axis=1
    )
    mixed = jnp.concatenate([mixed, jnp.zeros((12, lanes), F32)], axis=0).astype(BF)

    def correct(index, carry):
        columns = pl.ds(pl.multiple_of(index * slab, 128), slab)
        result = jnp.dot(mixed, whole[:, columns], preferred_element_type=F32)
        for group in range(slab // 128):
            extra_rows[pl.ds(index * (slab // 128) + group, 4, stride=width // 128), :] = result[
                :4, group * 128 : (group + 1) * 128
            ]
        return carry

    lax.fori_loop(0, slabs, correct, 0)

    @pl.when(is_relay)
    def _():
        took(moved.at[pl.ds(0, RELAYS - 1)], moved_recv)
        sent(picked.at[pl.ds(0, replicas - 1)], moved_send)
        sent(spread.at[pl.ds(0, RELAYS - 1)], spread_send)

    @pl.when(jnp.logical_not(is_relay))
    def _():
        took(moved, moved_recv)
        sent(spread.at[pl.ds(0, RELAYS)], spread_send)

    is_out = table_ref[dp] >= half_blocks
    main = summed[:block_rows, :]
    grads_ref[...] = jnp.where(is_out, main + extra_rows[...], main) / loss_scale

    @pl.when(me < hop)
    def _():
        rows_copy().wait_send()

    @pl.when(valid)
    def _():
        sent(prod.at[0, pl.ds(0, replicas - 1)], prod_send)

    @pl.when(me < half)
    def _():
        sent(whole.at[pl.ds(0, 3 * tall), pl.ds(0, wide)], pass_send)

    sent(uv_out.at[pl.ds(0, sections - 1)], uv_send)
    for section in range(sections):

        @pl.when(me != section)
        def _(section=section):
            p_copy(section).wait_send()

    for section in range(1, sections):

        @pl.when(me == section)
        def _(section=section):
            sent(prod.at[pl.ds(0, sections - 1), pl.ds(0, 4 * section)], gather_send)
            copies = len(slice_targets(section))
            sent(whole.at[pl.ds(0, copies * tall), pl.ds(0, wide)], slice_send)

        @pl.when(me < section)
        def _(section=section):
            sent(whole.at[pl.ds(0, 3 * tall), pl.ds(0, wide)], wide_send.at[section])
            pair_copy(section).wait_send()

    for far in range(ND):
        half_copy(far).wait_send()
        sent(y_got.at[far, pl.ds(1, NY - 1)], y_send.at[far])
        if far:
            z_copy(far).wait_send()


def vmem():
    return pl.BlockSpec(memory_space=pltpu.VMEM)


def smem():
    return pl.BlockSpec(memory_space=pltpu.SMEM)


def hbm():
    return pl.BlockSpec(memory_space=pl.ANY)


def run_drain(table, old, plan, inputs, base, turned, weight_out, first, second):
    tokens, width = inputs.shape
    rank = turned.shape[0]
    sections = SECTIONS
    replicas = ND * NY * NC
    tok_rows = tokens // sections
    lanes = sections * rank
    half_blocks = replicas // 2
    rows = width * rank // half_blocks // 128
    extra = rank * lanes // 128 // half_blocks
    relay_rows = first.shape[2]
    dma = pltpu.SemaphoreType.DMA
    full = (rows + extra, 128)
    per_section = dma((sections,))
    per_z = dma((ND,))
    return pl.pallas_call(
        drain_kernel,
        out_shape=(
            pltpu.VMEM((sections, tok_rows, width), BF),
            jax.ShapeDtypeStruct((rows, 128), F32),
            jax.ShapeDtypeStruct((RELAYS, 2 * relay_rows, 128), BF),
        ),
        in_specs=[smem()] * 3 + [hbm()] * 2 + [vmem()] * 4,
        out_specs=(vmem(), vmem(), vmem()),
        scratch_shapes=[
            pltpu.VMEM((tokens, width), BF),
            pltpu.VMEM((sections, tok_rows, width), BF),
            pltpu.VMEM((tokens, rank), F32),
            pltpu.VMEM((tokens, rank), F32),
            pltpu.VMEM((tokens, rank), BF),
            pltpu.VMEM((rank // NY, width), BF),
            pltpu.VMEM((8, 128), BF),
            pltpu.VMEM((sections, 32, 8, 128), BF),
            pltpu.VMEM((sections, tok_rows, 2 * rank), BF),
            pltpu.VMEM((sections, tok_rows, 2 * rank), BF),
            pltpu.VMEM((tok_rows, lanes), F32),
            pltpu.VMEM((RELAYS, 4 * relay_rows, 128), BF),
            pltpu.VMEM((replicas, 4 * relay_rows, 128), BF),
            pltpu.VMEM((replicas, 2 * relay_rows, 128), BF),
            pltpu.VMEM((lanes, width), BF),
            pltpu.VMEM((sections, tok_rows, lanes), BF),
            pltpu.VMEM((tokens, lanes), BF),
            pltpu.VMEM((width, rank), F32),
            pltpu.VMEM((half_blocks * rows, 128), F32),
            pltpu.VMEM((half_blocks * extra, 128), F32),
            pltpu.VMEM((rows, 128), F32),
            pltpu.VMEM((replicas, *full), F32),
            pltpu.VMEM((ND, NY, *full), BF),
            pltpu.VMEM((ND, NY, *full), BF),
            pltpu.VMEM((ND, NY, *full), BF),
            pltpu.VMEM((ND, NY, *full), BF),
            pltpu.VMEM((ND, *full), BF),
            pltpu.VMEM((ND, *full), BF),
            pltpu.VMEM(full, F32),
            dma((2, 6)),
            dma,
            dma,
            dma,
            dma,
            dma,
            dma,
            dma,
            per_section,
            per_section,
            dma,
            dma,
            dma,
            dma,
            dma,
            dma,
            per_section,
            dma,
            per_section,
            per_section,
            per_section,
            per_section,
            per_z,
            per_z,
            per_z,
            per_z,
            per_z,
            per_z,
        ],
        compiler_params=pltpu.CompilerParams(
            collective_id=0, has_side_effects=True, vmem_limit_bytes=60 * 2**20
        ),
        name="drain",
    )(table, old, plan, inputs, base, turned, weight_out, first, second)


def per_device(
    activations,
    loss_grads,
    adapter_in,
    adapter_out,
    first_moment,
    second_moment,
    old_owner,
    new_owner,
    plan,
):
    replicas = lax.axis_size(DP)
    micro_count, tok_rows, width = activations.shape[1:]
    rank = adapter_in.shape[2]
    tokens = micro_count * tok_rows
    inputs = activations[0].reshape(tokens, width)
    owners_old = old_owner[0]
    owners_new = new_owner[0]
    block_len = first_moment.shape[2] // 2
    block_rows = block_len // 128
    relay_rows = block_rows // RELAYS
    replica_ids = jnp.arange(replicas, dtype=jnp.int32)
    matches = owners_new[None, :] == replica_ids[:, None]
    table = jnp.sum(jnp.where(matches, replica_ids[None, :], 0), axis=1)
    emitted, grads, moved = run_drain(
        table.astype(jnp.int32),
        owners_old,
        plan,
        inputs,
        loss_grads,
        adapter_in[0].T,
        adapter_out[0],
        first_moment.reshape(2, RELAYS, relay_rows, 128),
        second_moment.reshape(2, RELAYS, relay_rows, 128),
    )
    first_old = moved[:, :relay_rows].astype(F32).reshape(block_rows, 128)
    second_old = moved[:, relay_rows:].astype(F32).reshape(block_rows, 128)
    first_next = beta_one * first_old + (1.0 - beta_one) * grads
    second_next = beta_two * second_old + (1.0 - beta_two) * grads * grads
    update = (
        first_next
        / (1.0 - beta_one**adam_step)
        / (jnp.sqrt(second_next / (1.0 - beta_two**adam_step)) + adam_eps)
    )
    shape = (1, 1, block_len)
    return (
        emitted[None],
        update.reshape(shape),
        first_next.reshape(shape),
        second_next.reshape(shape),
    )


def solution(mesh):
    torus = Mesh(
        mesh.devices.reshape(mesh.shape["section"], ND, NY, NC), ("section", "dp_0", "dp_1", "dp_2")
    )
    in_specs = (
        P("section", None, DP, None),
        P(None, DP, None),
        P("section", None, None),
        P("section", None, None),
        P("section", DP, None),
        P("section", DP, None),
        P("section", None),
        P("section", None),
        P(),
    )
    out_specs = (
        P("section", None, DP, None),
        P("section", DP, None),
        P("section", DP, None),
        P("section", DP, None),
    )
    return jax.shard_map(
        per_device, mesh=torus, in_specs=in_specs, out_specs=out_specs, check_vma=False
    )
```
